32 devices in a mesh: blk: 16 (over z, x, core), cat: 2 (over y).
Axes of the slice: x: 2, y: 2, z: 4, core: 2. Of those that a mesh axis runs over, the one named last changes fastest.
Arguments:
- item_content: bfloat16 [32768, 512], P('blk', 'cat'), may hold values from -6 to 6
- projection: bfloat16 [512, 256], replicated, may hold values from -0.06591797 to 0.06591797
- send_order: int32 [32, 1024], P(('blk', 'cat')), may hold values from 0 to 1023, each once within a row
- user_factors: float32 [16384, 256], P(('blk', 'cat')), may hold values from -1.5 to 1.5
- ratings: int32 [16384, 4, 1024], P(('blk', 'cat')), may hold values from 0 to 5, as said below
Outputs:
- users_out: float32 [16384, 256], P(('blk', 'cat'))
- items_out: float32 [32768, 256], P(('blk', 'cat'))
The draws below stay inside these ranges and needn't reach their ends.
Inputs may be any that keep to these rules, and one draw needn't show every extreme that they name: `send_order`: each row is a permutation of 0 .. 1023. `ratings`: 0 means no rating, 1 to 5 a rating.
All inputs are finite; a program needn't handle non-finite values.
Results may differ from the reference program's by a relative error of at most 0.0003.
Values may be sent and summed in bfloat16 or wider, within the bound.
A program may use at most 64 MiB of HBM per device.

```python
import jax
import jax.numpy as jnp
from jax import lax

R = 256
C = 512
U_DEV = 512
ITEM_DEV = 1024
ROUNDS = 4
USERS = 16384
ITEMS = 32768
N_BLK = 16
N_CAT = 2
DEVICES = 32


def draw_ratings(key, part):
    shape = (USERS, ROUNDS, ITEM_DEV)
    levels = jax.random.randint(jax.random.fold_in(key, 11), shape, 1, 6)
    present = jax.random.randint(jax.random.fold_in(key, 12), shape, 0, 3)
    return jnp.where(present == 0, levels, 0).astype(jnp.int32)


def block_scale(rng, shape, cuts, smallest, largest):
    gain, own = 1.0, jax.random.fold_in(rng, 6)
    for axis_at, blocks in cuts:
        steps = jnp.exp(jax.random.uniform(jax.random.fold_in(own, axis_at), (blocks,), jnp.float32, smallest / len(cuts), largest / len(cuts)))
        gain = gain * jnp.repeat(steps, shape[axis_at] // blocks).reshape([-1 if axis == axis_at else 1 for axis in range(len(shape))])
    return gain


def noise(key, shape, width, bound, cuts=(), held_as=jnp.bfloat16):
    gain = block_scale(key, shape, cuts, -0.22, 0.18) if cuts else 1.0
    drawn = jax.random.normal(key, shape, jnp.float32) * width * gain
    return jnp.minimum(jnp.maximum(drawn, -bound), bound).astype(held_as)


def setup_inputs(seed: int = 0) -> dict:
    keys = jax.random.split(jax.random.key(seed), 6)
    item_content = noise(keys[0], (ITEMS, C), 1.0, 6.0, ((0, 16), (1, 2)))
    projection = noise(keys[1], (C, R), 0.011, 0.06591797)
    send_order = jax.vmap(lambda own: jax.random.permutation(own, ITEM_DEV))(jax.random.split(keys[2], DEVICES)).reshape((DEVICES, ITEM_DEV)).astype(jnp.int32)
    user_factors = noise(keys[3], (USERS, R), 0.25, 1.5, ((0, 32),), jnp.float32)
    ratings = draw_ratings(jax.random.fold_in(keys[5], 71), 0)
    return dict(item_content=item_content, projection=projection, send_order=send_order, user_factors=user_factors, ratings=ratings)


learn_rate = 0.004
shrink = 0.05


def reference(item_content, projection, send_order, user_factors, ratings):
    projected = jnp.dot(item_content, projection, preferred_element_type=jnp.float32)
    blocks = projected.reshape(N_BLK, N_CAT, ITEM_DEV, R)
    orders = send_order.reshape(N_BLK, N_CAT, ITEM_DEV)
    dealt = jnp.take_along_axis(blocks, orders[..., None], axis=2)
    share = ITEM_DEV // N_BLK
    items = dealt.reshape(N_BLK, N_CAT, N_BLK, share, R).transpose(2, 1, 0, 3, 4).reshape(N_BLK, N_CAT, ITEM_DEV, R)
    users = user_factors.reshape(N_BLK, N_CAT, U_DEV, R)
    values_all = ratings.reshape(N_BLK, N_CAT, U_DEV, ROUNDS, ITEM_DEV)
    for round_index in range(ROUNDS):
        if round_index > 0:
            items = jnp.roll(items, 1, axis=0)
        values = values_all[:, :, :, round_index, :].astype(jnp.float32)
        masks = jnp.where(values > 0, jnp.float32(1.0), jnp.float32(0.0))
        guess = jnp.einsum("bcur,bcir->bcui", users, items, precision=lax.Precision.HIGHEST)
        errors = masks * (values - guess)
        user_grad = jnp.einsum("bcui,bcir->bcur", errors, items, precision=lax.Precision.HIGHEST)
        item_grad = jnp.einsum("bcui,bcur->bcir", errors, users, precision=lax.Precision.HIGHEST)
        users, items = (users + learn_rate * (user_grad - shrink * users),
                        items + learn_rate * (item_grad - shrink * items))
    return users.reshape(USERS, R), items.reshape(ITEMS, R)
```

```python
import functools
import jax
import jax.numpy as jnp
from jax import lax
from jax.experimental import pallas as pl
from jax.experimental.pallas import tpu as pltpu
from jax.sharding import PartitionSpec as P

learn_rate = 0.004
shrink = 0.05
LEVELS = 32000.0
STEPS = 20.0
CHUNK = 256
LANES = 128
MESH = pl.DeviceIdType.MESH


def split(value):
    high = value.astype(jnp.bfloat16)
    return high, (value - high.astype(jnp.float32)).astype(jnp.bfloat16)


def product(left, right, dims):
    def one(a, b):
        return lax.dot_general(a, b, (dims, ((), ())), preferred_element_type=jnp.float32)

    return one(left[0], right[0]) + (one(left[0], right[1]) + one(left[1], right[0]))


def code_of(largest):
    return jnp.ceil(jnp.log(jnp.maximum(largest, 1e-30)) * STEPS)


def step_of(code):
    return jnp.exp(code * (1.0 / STEPS)) * (1.0 / LEVELS)


def coded(value, step):
    return jnp.floor(value * (1.0 / step) + 0.5).astype(jnp.int32).astype(jnp.int16)


def decoded(value, step):
    return value.astype(jnp.int32).astype(jnp.float32) * step


def rounds_kernel(
    rounds, items_in, users_in, ratings_in, users_out, items_out,
    users, ratings, sent, sent_steps, got, got_steps, load_sem, send_sem, recv_sem,
):
    size = lax.axis_size("blk")
    me = lax.axis_index("blk")
    right, left = lax.rem(me + 1, size), lax.rem(me + size - 1, size)
    n_users, rank = users.shape
    n_items = items_in.shape[0]
    chunk = got.shape[2]
    tiles = n_items // LANES
    loads = [
        pltpu.make_async_copy(users_in, users, load_sem.at[0]),
        pltpu.make_async_copy(ratings_in, ratings, load_sem.at[1]),
    ]
    for load in loads:
        load.start()
    barrier = pltpu.get_barrier_semaphore()
    pl.semaphore_signal(barrier, inc=1, device_id={"blk": left}, device_id_type=MESH)
    pl.semaphore_wait(barrier, 1)
    for load in loads:
        load.wait()

    def moves(t, n):
        return [
            pltpu.make_async_remote_copy(
                src_ref=src.at[t, n],
                dst_ref=dst.at[t, n],
                send_sem=send_sem.at[t, n, k],
                recv_sem=recv_sem.at[t, n, k],
                device_id={"blk": right},
                device_id_type=MESH,
            )
            for k, (src, dst) in enumerate([(sent, got), (sent_steps, got_steps)])
        ]

    for t in range(rounds):
        now = users[...]
        user_parts = split(now)
        user_grad = jnp.zeros(now.shape, jnp.float32)
        for n in range(n_items // chunk):
            at = pl.ds(n * chunk, chunk)
            if t == 0:
                old = items_in[at, :]
            else:
                for move in moves(t - 1, n):
                    move.wait_recv()
                old = decoded(got[t - 1, n], got_steps[t - 1, n])
            old_parts = split(old)
            guess = product(user_parts, old_parts, ((1,), (1,)))
            values = jnp.concatenate(
                [
                    ratings[pl.ds((n * (chunk // LANES) + j) * rounds + t, n_users, stride=tiles * rounds), :]
                    for j in range(chunk // LANES)
                ],
                axis=1,
            ).astype(jnp.float32)
            errors = jnp.where(values > 0.0, values - guess, 0.0)
            error_parts = split(errors)
            item_grad = product(error_parts, user_parts, ((0,), (0,)))
            new = old + learn_rate * (item_grad - shrink * old)
            if t < rounds - 1:
                step = jnp.maximum(jnp.max(jnp.abs(new), axis=0, keepdims=True), 1e-30) * (1.0 / LEVELS)
                sent[t, n] = coded(new, step)
                sent_steps[t, n] = step
                for move in moves(t, n):
                    move.start()
            else:
                items_out[at, :] = new
            user_grad += product(error_parts, old_parts, ((1,), (0,)))
        now = now + learn_rate * (user_grad - shrink * now)
        if t < rounds - 1:
            users[...] = now
        else:
            users_out[...] = now
    for t in range(rounds - 1):
        for n in range(n_items // chunk):
            for move in moves(t, n):
                move.wait_send()


def all_rounds(items, users, ratings):
    n_users, rounds, n_items = ratings.shape
    rank = users.shape[1]
    chunk = min(CHUNK, n_items)
    chunks = n_items // chunk
    view = ratings.reshape(n_users, rounds, n_items // LANES, LANES).transpose(0, 2, 1, 3).reshape(-1, LANES)
    return pl.pallas_call(
        functools.partial(rounds_kernel, rounds),
        in_specs=[
            pl.BlockSpec(memory_space=pltpu.VMEM),
            pl.BlockSpec(memory_space=pl.ANY),
            pl.BlockSpec(memory_space=pl.ANY),
        ],
        out_specs=[pl.BlockSpec(memory_space=pltpu.VMEM)] * 2,
        out_shape=[
            jax.ShapeDtypeStruct(users.shape, jnp.float32),
            jax.ShapeDtypeStruct(items.shape, jnp.float32),
        ],
        scratch_shapes=[
            pltpu.VMEM(users.shape, jnp.float32),
            pltpu.VMEM(view.shape, jnp.int32),
            pltpu.VMEM((rounds - 1, chunks, chunk, rank), jnp.int16),
            pltpu.VMEM((rounds - 1, chunks, 1, rank), jnp.float32),
            pltpu.VMEM((rounds - 1, chunks, chunk, rank), jnp.int16),
            pltpu.VMEM((rounds - 1, chunks, 1, rank), jnp.float32),
            pltpu.SemaphoreType.DMA((2,)),
            pltpu.SemaphoreType.DMA((rounds - 1, chunks, 2)),
            pltpu.SemaphoreType.DMA((rounds - 1, chunks, 2)),
        ],
        cost_estimate=pl.CostEstimate(
            flops=18 * n_users * n_items * rank * rounds, bytes_accessed=12 << 20, transcendentals=0
        ),
        compiler_params=pltpu.CompilerParams(
            vmem_limit_bytes=48 << 20, collective_id=0, has_side_effects=True
        ),
        name="sgd_rounds",
    )(items, users, view)


def project(item_content, projection):
    def dot(rows, weights):
        return jnp.dot(rows, weights, preferred_element_type=jnp.float32)

    if lax.axis_size("cat") != 2:
        rows = lax.all_to_all(item_content, "cat", split_axis=0, concat_axis=1, tiled=True)
        return dot(rows, projection)
    me = lax.axis_index("cat")
    rows, width = item_content.shape[0] // 2, item_content.shape[1]
    other = 1 - me
    theirs = lax.dynamic_slice_in_dim(item_content, other * rows, rows)
    got = lax.ppermute(theirs, "cat", [(0, 1), (1, 0)])
    mine = lax.dynamic_slice_in_dim(item_content, me * rows, rows)
    near = dot(mine, lax.dynamic_slice_in_dim(projection, me * width, width))
    return near + dot(got, lax.dynamic_slice_in_dim(projection, other * width, width))


def body(item_content, projection, send_order, user_factors, ratings):
    size = lax.axis_size("blk")
    owned = project(item_content, projection)
    ordered = owned.at[send_order[0]].get(mode="promise_in_bounds")
    dealt = ordered.reshape(size, -1, ordered.shape[1])
    share = dealt.shape[1]
    code = code_of(jnp.max(jnp.abs(dealt), axis=1, keepdims=True))
    sent = jnp.concatenate(
        [coded(dealt, step_of(code)), code.astype(jnp.int32).astype(jnp.int16)], axis=1
    )
    got = lax.all_to_all(sent, "blk", split_axis=0, concat_axis=0, tiled=True)
    got = got.astype(jnp.int32).astype(jnp.float32)
    items = (got[:, :share] * step_of(got[:, share:])).reshape(owned.shape)
    return tuple(all_rounds(items, user_factors, ratings))


def solution(mesh):
    placed = (
        P("blk", "cat"),
        P(),
        P(("blk", "cat"), None),
        P(("blk", "cat"), None),
        P(("blk", "cat"), None, None),
    )
    return jax.shard_map(
        body,
        mesh=mesh,
        in_specs=placed,
        out_specs=(P(("blk", "cat"), None), P(("blk", "cat"), None)),
        check_vma=False,
    )
```

```python
import functools
import jax
import jax.numpy as jnp
from jax import lax
from jax.experimental import pallas as pl
from jax.experimental.pallas import tpu as pltpu
from jax.sharding import PartitionSpec as P

learn_rate = 0.004
shrink = 0.05
LEVELS = 32000.0
CHUNK = 256
FRONT = 128
LANES = 128
MESH = pl.DeviceIdType.MESH


def split(value):
    high = value.astype(jnp.bfloat16)
    return high, (value - high.astype(jnp.float32)).astype(jnp.bfloat16)


def dot(left, right, dims=((1,), (0,))):
    return lax.dot_general(left, right, (dims, ((), ())), preferred_element_type=jnp.float32)


def product(left, right, dims):
    return dot(left[0], right[0], dims) + (dot(left[0], right[1], dims) + dot(left[1], right[0], dims))


def steps_of(value, axis):
    return jnp.maximum(jnp.max(jnp.abs(value), axis=axis, keepdims=True), 1e-30) * (1.0 / LEVELS)


def coded(value, step):
    return jnp.floor(value * (1.0 / step) + 0.5).astype(jnp.int32).astype(jnp.int16)


def decoded(value, step):
    return value.astype(jnp.int32).astype(jnp.float32) * step


def paired(index, turn, count):
    if count & (count - 1):
        return lax.rem(turn - index + count, count)
    result, bit = index, 1
    while bit < count:
        if turn & bit:
            result = result + bit * (1 - 2 * lax.rem(lax.div(index, bit), 2))
        bit *= 2
    return result


def far_first(count):
    half = count // 2
    return list(range(half, count)) + list(range(half - 1, -1, -1))


def kernel(
    rounds, content_in, weights_in, order_in, users_in, ratings_in, users_out, items_out,
    content, weights, orders, column, near, far_sent, far_got,
    deal_sent, deal_steps, dealt, dealt_steps,
    users, ratings, sent, sent_steps, got, got_steps,
    load_sem, order_send, order_recv, far_send, far_recv, deal_send, deal_recv, send_sem, recv_sem,
):
    size, cats = lax.axis_size("blk"), lax.axis_size("cat")
    me, cat = lax.axis_index("blk"), lax.axis_index("cat")
    n_users, rank = users.shape
    n_items, width = content.shape[1:]
    share = n_items // size
    loads = [
        pltpu.make_async_copy(src, dst, load_sem.at[k])
        for k, (src, dst) in enumerate(
            [
                (order_in, orders.at[0]),
                (content_in, content),
                (weights_in, weights),
                (users_in, users),
                (ratings_in, ratings),
            ]
        )
    ]
    for load in loads:
        load.start()
    barrier = pltpu.get_barrier_semaphore()
    for k in range(1, cats):
        pl.semaphore_signal(barrier, inc=1, device_id={"cat": lax.rem(cat + k, cats)}, device_id_type=MESH)

    def greet(k, carry):
        pl.semaphore_signal(barrier, inc=1, device_id={"blk": lax.rem(me + k, size)}, device_id_type=MESH)
        return carry

    lax.fori_loop(1, size, greet, 0)

    front = far_sent.shape[2]
    fronts = n_items // front
    strata = front // share
    turns = far_first(fronts)

    def spread(slot):
        row = orders[slot].astype(jnp.float32)
        column[slot] = jnp.transpose(jnp.broadcast_to(row, (LANES, n_items)))

    def picked(slot, block, group):
        at = column[slot, pl.ds(pl.multiple_of(group * front, front), front), :]
        lane = lax.broadcasted_iota(jnp.int32, (front, LANES), 1).astype(jnp.float32)
        hot = jnp.concatenate(
            [jnp.where(at == lane + float(j * LANES), 1.0, 0.0).astype(jnp.bfloat16) for j in range(n_items // LANES)],
            axis=1,
        )
        return dot(hot, content[block]).astype(jnp.bfloat16)

    def near_part(n):
        group = paired(lax.div(me, strata), turns[n], fronts)
        near[n] = dot(picked(0, cat, group), weights[cat])

    loads[0].wait()
    spread(0)
    loads[1].wait()
    loads[2].wait()
    for n in range(fronts // 2):
        near_part(n)
    pl.semaphore_wait(barrier, size - 1 + cats - 1)

    def order_move(k):
        return pltpu.make_async_remote_copy(
            src_ref=order_in,
            dst_ref=orders.at[k],
            send_sem=order_send.at[k - 1],
            recv_sem=order_recv.at[k - 1],
            device_id={"cat": lax.rem(cat + k, cats)},
            device_id_type=MESH,
        )

    def far_move(k, n):
        return pltpu.make_async_remote_copy(
            src_ref=far_sent.at[k - 1, n],
            dst_ref=far_got.at[k - 1, n],
            send_sem=far_send.at[k - 1, n],
            recv_sem=far_recv.at[k - 1, n],
            device_id={"cat": lax.rem(cat + k, cats)},
            device_id_type=MESH,
        )

    def deal_moves(stratum, source, target):
        return [
            pltpu.make_async_remote_copy(
                src_ref=src.at[stratum],
                dst_ref=dst.at[source],
                send_sem=deal_send.at[stratum, k],
                recv_sem=deal_recv.at[source, k],
                device_id={"blk": target},
                device_id_type=MESH,
            )
            for k, (src, dst) in enumerate([(deal_sent, dealt), (deal_steps, dealt_steps)])
        ]

    for k in range(1, cats):
        order_move(k).start()
    for n in range(fronts // 2, fronts):
        near_part(n)
    for k in range(1, cats):
        order_move(cats - k).wait_recv()
        spread(cats - k)
        block = lax.rem(cat + k, cats)
        for n in range(fronts):
            group = paired(lax.div(me, strata), turns[n], fronts)
            far_sent[k - 1, n] = picked(cats - k, block, group)
            far_move(k, n).start()
    for n in range(fronts):
        group = paired(lax.div(me, strata), turns[n], fronts)
        owned = near[n]
        for k in range(1, cats):
            far_move(k, n).wait_recv()
            owned += dot(far_got[k - 1, n], weights[lax.rem(cat + cats - k, cats)])
        owned = owned.reshape(strata, share, rank)
        step = steps_of(owned, 1)
        codes = coded(owned, step)
        first = group * strata
        if turns[n] and fronts & (fronts - 1) == 0:
            deal_sent[pl.ds(first, strata)] = codes
            deal_steps[pl.ds(first, strata)] = step
            for i in range(strata):
                for move in deal_moves(first + i, me, first + i):
                    move.start()
        else:
            for i in range(strata):
                stratum = first + i

                @pl.when(stratum == me)
                def _():
                    dealt[me] = codes[i]
                    dealt_steps[me] = step[i]

                @pl.when(stratum != me)
                def _():
                    deal_sent[stratum] = codes[i]
                    deal_steps[stratum] = step[i]
                    for move in deal_moves(stratum, me, stratum):
                        move.start()

    right = lax.rem(me + 1, size)
    chunk = got.shape[2]
    chunks = n_items // chunk
    per = chunk // share
    order = far_first(chunks)
    tiles = n_items // LANES

    def moves(t, n):
        return [
            pltpu.make_async_remote_copy(
                src_ref=src.at[t, n],
                dst_ref=dst.at[t, n],
                send_sem=send_sem.at[t, n, k],
                recv_sem=recv_sem.at[t, n, k],
                device_id={"blk": right},
                device_id_type=MESH,
            )
            for k, (src, dst) in enumerate([(sent, got), (sent_steps, got_steps)])
        ]

    loads[3].wait()
    loads[4].wait()
    for t in range(rounds):
        now = users[...]
        user_parts = split(now)
        user_grad = jnp.zeros(now.shape, jnp.float32)
        start = lax.rem(me - t + size, size)
        for n in range(chunks):
            place = paired(lax.div(start, per), order[n], chunks)
            if t == 0:
                for i in range(per):
                    source = place * per + i

                    @pl.when(source != me)
                    def _():
                        for move in deal_moves(source, source, source):
                            move.wait_recv()

                here = pl.ds(place * per, per)
                old = decoded(dealt[here], dealt_steps[here]).reshape(chunk, rank)
            else:
                for move in moves(t - 1, n):
                    move.wait_recv()
                old = decoded(got[t - 1, n], got_steps[t - 1, n])
            old_parts = split(old)
            guess = product(user_parts, old_parts, ((1,), (1,)))
            first = place * (chunk // LANES)
            values = jnp.concatenate(
                [
                    ratings[pl.ds((first + j) * rounds + t, n_users, stride=tiles * rounds), :]
                    for j in range(chunk // LANES)
                ],
                axis=1,
            ).astype(jnp.float32)
            errors = jnp.where(values > 0.0, values - guess, 0.0)
            error_parts = split(errors)
            item_grad = product(error_parts, user_parts, ((0,), (0,)))
            new = old + learn_rate * (item_grad - shrink * old)
            if t < rounds - 1:
                step = steps_of(new, 0)
                sent[t, n] = coded(new, step)
                sent_steps[t, n] = step
                for move in moves(t, n):
                    move.start()
            else:
                items_out[pl.ds(pl.multiple_of(place * chunk, chunk), chunk), :] = new
            user_grad += product(error_parts, old_parts, ((1,), (0,)))
        now = now + learn_rate * (user_grad - shrink * now)
        if t < rounds - 1:
            users[...] = now
        else:
            users_out[...] = now

    for k in range(1, cats):
        order_move(k).wait_send()
        for n in range(fronts):
            far_move(k, n).wait_send()

    def settle(stratum, carry):
        @pl.when(stratum != me)
        def _():
            for move in deal_moves(stratum, me, stratum):
                move.wait_send()

        return carry

    lax.fori_loop(0, size, settle, 0)
    for t in range(rounds - 1):
        for n in range(chunks):
            for move in moves(t, n):
                move.wait_send()


def body(item_content, projection, send_order, user_factors, ratings):
    size, cats = lax.axis_size("blk"), lax.axis_size("cat")
    n_users, rounds, n_items = ratings.shape
    width, rank = item_content.shape[1], user_factors.shape[1]
    share = n_items // size
    chunk, front = max(CHUNK, share), max(FRONT, share)
    chunks, fronts = n_items // chunk, n_items // front
    view = ratings.reshape(n_users, rounds, n_items // LANES, LANES).transpose(0, 2, 1, 3).reshape(-1, LANES)
    dma = pltpu.SemaphoreType.DMA
    return tuple(
        pl.pallas_call(
            functools.partial(kernel, rounds),
            in_specs=[pl.BlockSpec(memory_space=pl.ANY)] * 5,
            out_specs=[pl.BlockSpec(memory_space=pltpu.VMEM)] * 2,
            out_shape=[
                jax.ShapeDtypeStruct((n_users, rank), jnp.float32),
                jax.ShapeDtypeStruct((n_items, rank), jnp.float32),
            ],
            scratch_shapes=[
                pltpu.VMEM((cats, n_items, width), jnp.bfloat16),
                pltpu.VMEM((cats, width, rank), jnp.bfloat16),
                pltpu.VMEM((cats, 1, n_items), jnp.int32),
                pltpu.VMEM((cats, n_items, LANES), jnp.float32),
                pltpu.VMEM((fronts, front, rank), jnp.float32),
                pltpu.VMEM((cats - 1, fronts, front, width), jnp.bfloat16),
                pltpu.VMEM((cats - 1, fronts, front, width), jnp.bfloat16),
                pltpu.VMEM((size, share, rank), jnp.int16),
                pltpu.VMEM((size, 1, rank), jnp.float32),
                pltpu.VMEM((size, share, rank), jnp.int16),
                pltpu.VMEM((size, 1, rank), jnp.float32),
                pltpu.VMEM((n_users, rank), jnp.float32),
                pltpu.VMEM(view.shape, jnp.int32),
                pltpu.VMEM((rounds - 1, chunks, chunk, rank), jnp.int16),
                pltpu.VMEM((rounds - 1, chunks, 1, rank), jnp.float32),
                pltpu.VMEM((rounds - 1, chunks, chunk, rank), jnp.int16),
                pltpu.VMEM((rounds - 1, chunks, 1, rank), jnp.float32),
                dma((5,)),
                dma((cats - 1,)),
                dma((cats - 1,)),
                dma((cats - 1, fronts)),
                dma((cats - 1, fronts)),
                dma((size, 2)),
                dma((size, 2)),
                dma((rounds - 1, chunks, 2)),
                dma((rounds - 1, chunks, 2)),
            ],
            cost_estimate=pl.CostEstimate(
                flops=18 * n_users * n_items * rank * rounds, bytes_accessed=12 << 20, transcendentals=0
            ),
            compiler_params=pltpu.CompilerParams(
                vmem_limit_bytes=48 << 20, collective_id=0, has_side_effects=True
            ),
            name="stratified_sgd",
        )(
            item_content.reshape(cats, n_items, width),
            projection.reshape(cats, width, rank),
            send_order,
            user_factors,
            view,
        )
    )


def solution(mesh):
    placed = (
        P("blk", "cat"),
        P(),
        P(("blk", "cat"), None),
        P(("blk", "cat"), None),
        P(("blk", "cat"), None, None),
    )
    return jax.shard_map(
        body,
        mesh=mesh,
        in_specs=placed,
        out_specs=(P(("blk", "cat"), None), P(("blk", "cat"), None)),
        check_vma=False,
    )
```

```python
import functools
import jax
import jax.numpy as jnp
from jax import lax
from jax.experimental import pallas as pl
from jax.experimental.pallas import tpu as pltpu
from jax.sharding import PartitionSpec as P

learn_rate = 0.004
shrink = 0.05
LEVELS = 32000.0
CHUNK = 256
FRONT = 128
LANES = 128
MESH = pl.DeviceIdType.MESH


def split(value):
    high = value.astype(jnp.bfloat16)
    return high, (value - high.astype(jnp.float32)).astype(jnp.bfloat16)


def dot(left, right, dims=((1,), (0,))):
    return lax.dot_general(left, right, (dims, ((), ())), preferred_element_type=jnp.float32)


def product(left, right, dims):
    return dot(left[0], right[0], dims) + (dot(left[0], right[1], dims) + dot(left[1], right[0], dims))


def steps_of(value, axis):
    return jnp.maximum(jnp.max(jnp.abs(value), axis=axis, keepdims=True), 1e-30) * (1.0 / LEVELS)


def coded(value, step):
    return jnp.floor(value * (1.0 / step) + 0.5).astype(jnp.int32).astype(jnp.int16)


def decoded(value, step):
    return value.astype(jnp.int32).astype(jnp.float32) * step


def paired(index, turn, count):
    if count & (count - 1):
        return lax.rem(turn - index + count, count)
    result, bit = index, 1
    while bit < count:
        if turn & bit:
            result = result + bit * (1 - 2 * lax.rem(lax.div(index, bit), 2))
        bit *= 2
    return result


def far_first(count):
    half = count // 2
    return list(range(half, count)) + list(range(half - 1, -1, -1))


def near_first(count):
    return [count // 2] + list(range(count // 2 - 1, -1, -1)) + list(range(count // 2 + 1, count))


def unpacked_early(count):
    return count // 4


def kernel(
    rounds, content_in, weights_in, order_in, users_in, ratings_in, users_out, items_out,
    content, weights, orders, column, near, far_sent, far_got,
    deal_sent, deal_steps, dealt, dealt_steps,
    users, ratings, values, sent, sent_steps, got, got_steps,
    load_sem, order_send, order_recv, far_send, far_recv, deal_send, deal_recv, send_sem, recv_sem,
):
    size, cats = lax.axis_size("blk"), lax.axis_size("cat")
    me, cat = lax.axis_index("blk"), lax.axis_index("cat")
    n_users, rank = users.shape
    n_items, width = content.shape[1:]
    share = n_items // size
    loads = [
        pltpu.make_async_copy(src, dst, load_sem.at[k])
        for k, (src, dst) in enumerate(
            [
                (order_in, orders.at[0]),
                (content_in, content),
                (weights_in, weights),
                (users_in, users),
                (ratings_in, ratings),
            ]
        )
    ]
    for load in loads:
        load.start()
    barrier = pltpu.get_barrier_semaphore()
    for k in range(1, cats):
        pl.semaphore_signal(barrier, inc=1, device_id={"cat": lax.rem(cat + k, cats)}, device_id_type=MESH)

    def greet(k, carry):
        pl.semaphore_signal(barrier, inc=1, device_id={"blk": lax.rem(me + k, size)}, device_id_type=MESH)
        return carry

    lax.fori_loop(1, size, greet, 0)

    front = far_sent.shape[2]
    fronts = n_items // front
    strata = front // share
    turns = far_first(fronts)

    def spread(slot):
        row = orders[slot].astype(jnp.float32)
        column[slot] = jnp.transpose(jnp.broadcast_to(row, (LANES, n_items)))

    def picked(slot, block, group):
        at = column[slot, pl.ds(pl.multiple_of(group * front, front), front), :]
        lane = lax.broadcasted_iota(jnp.int32, (front, LANES), 1).astype(jnp.float32)
        hot = jnp.concatenate(
            [jnp.where(at == lane + float(j * LANES), 1.0, 0.0).astype(jnp.bfloat16) for j in range(n_items // LANES)],
            axis=1,
        )
        return dot(hot, content[block]).astype(jnp.bfloat16)

    def near_part(n):
        group = paired(lax.div(me, strata), turns[n], fronts)
        near[n] = dot(picked(0, cat, group), weights[cat])

    loads[0].wait()
    spread(0)
    loads[1].wait()
    loads[2].wait()
    for n in range(fronts // 2):
        near_part(n)
    pl.semaphore_wait(barrier, size - 1 + cats - 1)

    def order_move(k):
        return pltpu.make_async_remote_copy(
            src_ref=order_in,
            dst_ref=orders.at[k],
            send_sem=order_send.at[k - 1],
            recv_sem=order_recv.at[k - 1],
            device_id={"cat": lax.rem(cat + k, cats)},
            device_id_type=MESH,
        )

    def far_move(k, n):
        return pltpu.make_async_remote_copy(
            src_ref=far_sent.at[k - 1, n],
            dst_ref=far_got.at[k - 1, n],
            send_sem=far_send.at[k - 1, n],
            recv_sem=far_recv.at[k - 1, n],
            device_id={"cat": lax.rem(cat + k, cats)},
            device_id_type=MESH,
        )

    def deal_moves(stratum, source, target):
        return [
            pltpu.make_async_remote_copy(
                src_ref=src.at[stratum],
                dst_ref=dst.at[source],
                send_sem=deal_send.at[stratum, k],
                recv_sem=deal_recv.at[source, k],
                device_id={"blk": target},
                device_id_type=MESH,
            )
            for k, (src, dst) in enumerate([(deal_sent, dealt), (deal_steps, dealt_steps)])
        ]

    for k in range(1, cats):
        order_move(k).start()
    for n in range(fronts // 2, fronts):
        near_part(n)
    for k in range(1, cats):
        order_move(cats - k).wait_recv()
        spread(cats - k)
        block = lax.rem(cat + k, cats)
        for n in range(fronts):
            group = paired(lax.div(me, strata), turns[n], fronts)
            far_sent[k - 1, n] = picked(cats - k, block, group)
            far_move(k, n).start()
    def deal(n):
        group = paired(lax.div(me, strata), turns[n], fronts)
        owned = near[n]
        for k in range(1, cats):
            far_move(k, n).wait_recv()
            owned += dot(far_got[k - 1, n], weights[lax.rem(cat + cats - k, cats)])
        owned = owned.reshape(strata, share, rank)
        step = steps_of(owned, 1)
        codes = coded(owned, step)
        first = group * strata
        if turns[n] and fronts & (fronts - 1) == 0:
            deal_sent[pl.ds(first, strata)] = codes
            deal_steps[pl.ds(first, strata)] = step
            for i in range(strata):
                for move in deal_moves(first + i, me, first + i):
                    move.start()
        else:
            for i in range(strata):
                stratum = first + i

                @pl.when(stratum == me)
                def _():
                    dealt[me] = codes[i]
                    dealt_steps[me] = step[i]

                @pl.when(stratum != me)
                def _():
                    deal_sent[stratum] = codes[i]
                    deal_steps[stratum] = step[i]
                    for move in deal_moves(stratum, me, stratum):
                        move.start()

    right = lax.rem(me + 1, size)
    chunk = got.shape[2]
    chunks = n_items // chunk
    per = chunk // share
    order = near_first(chunks)
    tiles = n_items // LANES

    def moves(t, n):
        return [
            pltpu.make_async_remote_copy(
                src_ref=src.at[t, n],
                dst_ref=dst.at[t, n],
                send_sem=send_sem.at[t, n, k],
                recv_sem=recv_sem.at[t, n, k],
                device_id={"blk": right},
                device_id_type=MESH,
            )
            for k, (src, dst) in enumerate([(sent, got), (sent_steps, got_steps)])
        ]

    def unpack(piece):
        t, n = divmod(piece, chunks)
        for j in range(chunk // LANES):
            tile = n * (chunk // LANES) + j
            part = ratings[pl.ds(tile * rounds + t, n_users, stride=tiles * rounds), :]
            values[t, n, :, pl.ds(j * LANES, LANES)] = part.astype(jnp.float32).astype(jnp.bfloat16)

    def round_step(t, n, user_parts, kept, grads):
        place = paired(lax.div(lax.rem(me - t + size, size), per), order[n], chunks)
        if t == 0:
            for i in range(per):
                source = place * per + i

                @pl.when(source != me)
                def _():
                    for move in deal_moves(source, source, source):
                        move.wait_recv()

            here = pl.ds(place * per, per)
            old = decoded(dealt[here], dealt_steps[here]).reshape(chunk, rank)
        else:
            for move in moves(t - 1, n):
                move.wait_recv()
            old = decoded(got[t - 1, n], got_steps[t - 1, n])
        old_parts = split(old)
        guess = product(user_parts, old_parts, ((1,), (1,)))
        rated = values[t, place].astype(jnp.float32)
        error_parts = split(jnp.where(rated > 0.0, rated - guess, 0.0))
        if kept:
            grads.append(product(*kept.pop(), ((1,), (0,))))
        item_grad = product(error_parts, user_parts, ((0,), (0,)))
        new = old + learn_rate * (item_grad - shrink * old)
        if t < rounds - 1:
            step = steps_of(new, 0)
            sent[t, n] = coded(new, step)
            sent_steps[t, n] = step
        else:
            items_out[pl.ds(pl.multiple_of(place * chunk, chunk), chunk), :] = new
        if n < chunks - 1:
            kept.append((error_parts, old_parts))
        else:
            grads.append(product(error_parts, old_parts, ((1,), (0,))))
        if t < rounds - 1:
            for move in moves(t, n):
                move.start()

    loads[3].wait()
    loads[4].wait()
    pieces = list(range(rounds * chunks))

    def unpack_some(count):
        for piece in pieces[:count]:
            unpack(piece)
        del pieces[:count]

    early = unpacked_early(rounds * chunks)
    unpack_some(early)
    each = pl.cdiv(len(pieces), fronts)
    parts = fronts // chunks
    now = users[...]
    user_parts = split(now)
    kept, grads = [], []

    def first_round(n):
        round_step(0, n, user_parts, kept, grads)

    for n in range(fronts):
        deal(n)
        unpack_some(each)
        if n == fronts - 1 - parts:
            first_round(0)
    unpack_some(len(pieces))
    for n in range(1, chunks):
        first_round(n)
    for t in range(rounds):
        if t > 0:
            user_parts, grads = split(now), []
            for n in range(chunks):
                round_step(t, n, user_parts, kept, grads)
        now = now + learn_rate * (functools.reduce(jnp.add, grads) - shrink * now)
    users_out[...] = now

    for k in range(1, cats):
        order_move(k).wait_send()
        for n in range(fronts):
            far_move(k, n).wait_send()

    def settle(stratum, carry):
        @pl.when(stratum != me)
        def _():
            for move in deal_moves(stratum, me, stratum):
                move.wait_send()

        return carry

    lax.fori_loop(0, size, settle, 0)
    for t in range(rounds - 1):
        for n in range(chunks):
            for move in moves(t, n):
                move.wait_send()


def body(item_content, projection, send_order, user_factors, ratings):
    size, cats = lax.axis_size("blk"), lax.axis_size("cat")
    n_users, rounds, n_items = ratings.shape
    width, rank = item_content.shape[1], user_factors.shape[1]
    share = n_items // size
    chunk, front = max(CHUNK, share), max(FRONT, share)
    chunks, fronts = n_items // chunk, n_items // front
    view = ratings.reshape(n_users, rounds, n_items // LANES, LANES).transpose(0, 2, 1, 3).reshape(-1, LANES)
    dma = pltpu.SemaphoreType.DMA
    return tuple(
        pl.pallas_call(
            functools.partial(kernel, rounds),
            in_specs=[pl.BlockSpec(memory_space=pl.ANY)] * 5,
            out_specs=[pl.BlockSpec(memory_space=pltpu.VMEM)] * 2,
            out_shape=[
                jax.ShapeDtypeStruct((n_users, rank), jnp.float32),
                jax.ShapeDtypeStruct((n_items, rank), jnp.float32),
            ],
            scratch_shapes=[
                pltpu.VMEM((cats, n_items, width), jnp.bfloat16),
                pltpu.VMEM((cats, width, rank), jnp.bfloat16),
                pltpu.VMEM((cats, 1, n_items), jnp.int32),
                pltpu.VMEM((cats, n_items, LANES), jnp.float32),
                pltpu.VMEM((fronts, front, rank), jnp.float32),
                pltpu.VMEM((cats - 1, fronts, front, width), jnp.bfloat16),
                pltpu.VMEM((cats - 1, fronts, front, width), jnp.bfloat16),
                pltpu.VMEM((size, share, rank), jnp.int16),
                pltpu.VMEM((size, 1, rank), jnp.float32),
                pltpu.VMEM((size, share, rank), jnp.int16),
                pltpu.VMEM((size, 1, rank), jnp.float32),
                pltpu.VMEM((n_users, rank), jnp.float32),
                pltpu.VMEM(view.shape, jnp.int32),
                pltpu.VMEM((rounds, chunks, n_users, chunk), jnp.bfloat16),
                pltpu.VMEM((rounds - 1, chunks, chunk, rank), jnp.int16),
                pltpu.VMEM((rounds - 1, chunks, 1, rank), jnp.float32),
                pltpu.VMEM((rounds - 1, chunks, chunk, rank), jnp.int16),
                pltpu.VMEM((rounds - 1, chunks, 1, rank), jnp.float32),
                dma((5,)),
                dma((cats - 1,)),
                dma((cats - 1,)),
                dma((cats - 1, fronts)),
                dma((cats - 1, fronts)),
                dma((size, 2)),
                dma((size, 2)),
                dma((rounds - 1, chunks, 2)),
                dma((rounds - 1, chunks, 2)),
            ],
            cost_estimate=pl.CostEstimate(
                flops=18 * n_users * n_items * rank * rounds, bytes_accessed=12 << 20, transcendentals=0
            ),
            compiler_params=pltpu.CompilerParams(
                vmem_limit_bytes=48 << 20, collective_id=0, has_side_effects=True
            ),
            name="stratified_sgd",
        )(
            *[
                pltpu.with_memory_space_constraint(value, pltpu.HBM)
                for value in (
                    item_content.reshape(cats, n_items, width),
                    projection.reshape(cats, width, rank),
                    send_order,
                    user_factors,
                    view,
                )
            ]
        )
    )


def solution(mesh):
    placed = (
        P("blk", "cat"),
        P(),
        P(("blk", "cat"), None),
        P(("blk", "cat"), None),
        P(("blk", "cat"), None, None),
    )
    return jax.shard_map(
        body,
        mesh=mesh,
        in_specs=placed,
        out_specs=(P(("blk", "cat"), None), P(("blk", "cat"), None)),
        check_vma=False,
    )
```

```python
import functools
import jax
import jax.numpy as jnp
from jax import lax
from jax.experimental import pallas as pl
from jax.experimental.pallas import tpu as pltpu
from jax.sharding import PartitionSpec as P

learn_rate = 0.004
shrink = 0.05
LEVELS = 32000.0
CHUNK = 256
FRONT = 256
LANES = 128
MESH = pl.DeviceIdType.MESH


def split(value):
    high = value.astype(jnp.bfloat16)
    return high, (value - high.astype(jnp.float32)).astype(jnp.bfloat16)


def dot(left, right, dims=((1,), (0,))):
    return lax.dot_general(left, right, (dims, ((), ())), preferred_element_type=jnp.float32)


def product(left, right, dims):
    return dot(left[0], right[0], dims) + (dot(left[0], right[1], dims) + dot(left[1], right[0], dims))


def steps_of(value, axis):
    return jnp.maximum(jnp.max(jnp.abs(value), axis=axis, keepdims=True), 1e-30) * (1.0 / LEVELS)


def coded(value, step):
    return jnp.floor(value * (1.0 / step) + 0.5).astype(jnp.int32).astype(jnp.int16)


def decoded(value, step):
    return value.astype(jnp.int32).astype(jnp.float32) * step


def paired(index, turn, count):
    if count & (count - 1):
        return lax.rem(turn - index + count, count)
    result, bit = index, 1
    while bit < count:
        if turn & bit:
            result = result + bit * (1 - 2 * lax.rem(lax.div(index, bit), 2))
        bit *= 2
    return result


def far_first(count):
    half = count // 2
    return list(range(half, count)) + list(range(half - 1, -1, -1))


def near_first(count):
    return [count // 2] + list(range(count // 2 - 1, -1, -1)) + list(range(count // 2 + 1, count))


def unpacked_early(count):
    return count // 4


def kernel(
    rounds, content_in, weights_in, order_in, users_in, ratings_in, users_out, items_out,
    content, weights, orders, column, near, far_sent, far_got,
    deal_sent, deal_steps, dealt, dealt_steps,
    users, ratings, values, sent, sent_steps, got, got_steps,
    load_sem, order_send, order_recv, far_send, far_recv, deal_send, deal_recv, send_sem, recv_sem,
):
    size, cats = lax.axis_size("blk"), lax.axis_size("cat")
    me, cat = lax.axis_index("blk"), lax.axis_index("cat")
    n_users, rank = users.shape
    n_items, width = content.shape[1:]
    share = n_items // size
    loads = [
        pltpu.make_async_copy(src, dst, load_sem.at[k])
        for k, (src, dst) in enumerate(
            [
                (order_in, orders.at[0]),
                (content_in, content),
                (weights_in, weights),
                (users_in, users),
                (ratings_in, ratings),
            ]
        )
    ]
    for load in loads:
        load.start()
    barrier = pltpu.get_barrier_semaphore()
    for k in range(1, cats):
        pl.semaphore_signal(barrier, inc=1, device_id={"cat": lax.rem(cat + k, cats)}, device_id_type=MESH)

    def greet(k, carry):
        pl.semaphore_signal(barrier, inc=1, device_id={"blk": lax.rem(me + k, size)}, device_id_type=MESH)
        return carry

    lax.fori_loop(1, size, greet, 0)

    front = far_sent.shape[2]
    fronts = n_items // front
    strata = front // share
    turns = far_first(fronts)

    def spread(slot):
        row = orders[slot].astype(jnp.float32)
        column[slot] = jnp.transpose(jnp.broadcast_to(row, (LANES, n_items)))

    def picked(slot, block, group):
        at = column[slot, pl.ds(pl.multiple_of(group * front, front), front), :]
        lane = lax.broadcasted_iota(jnp.int32, (front, LANES), 1).astype(jnp.float32)
        hot = jnp.concatenate(
            [jnp.where(at == lane + float(j * LANES), 1.0, 0.0).astype(jnp.bfloat16) for j in range(n_items // LANES)],
            axis=1,
        )
        return dot(hot, content[block]).astype(jnp.bfloat16)

    def near_part(n):
        group = paired(lax.div(me, strata), turns[n], fronts)
        near[n] = dot(picked(0, cat, group), weights[cat])

    loads[0].wait()
    spread(0)
    loads[1].wait()
    loads[2].wait()
    for n in range(fronts // 2):
        near_part(n)
    pl.semaphore_wait(barrier, size - 1 + cats - 1)

    def order_move(k):
        return pltpu.make_async_remote_copy(
            src_ref=order_in,
            dst_ref=orders.at[k],
            send_sem=order_send.at[k - 1],
            recv_sem=order_recv.at[k - 1],
            device_id={"cat": lax.rem(cat + k, cats)},
            device_id_type=MESH,
        )

    def far_move(k, n):
        return pltpu.make_async_remote_copy(
            src_ref=far_sent.at[k - 1, n],
            dst_ref=far_got.at[k - 1, n],
            send_sem=far_send.at[k - 1, n],
            recv_sem=far_recv.at[k - 1, n],
            device_id={"cat": lax.rem(cat + k, cats)},
            device_id_type=MESH,
        )

    def deal_moves(stratum, source, target):
        return [
            pltpu.make_async_remote_copy(
                src_ref=src.at[stratum],
                dst_ref=dst.at[source],
                send_sem=deal_send.at[stratum, k],
                recv_sem=deal_recv.at[source, k],
                device_id={"blk": target},
                device_id_type=MESH,
            )
            for k, (src, dst) in enumerate([(deal_sent, dealt), (deal_steps, dealt_steps)])
        ]

    for k in range(1, cats):
        order_move(k).start()
    for n in range(fronts // 2, fronts):
        near_part(n)
    for k in range(1, cats):
        order_move(cats - k).wait_recv()
        spread(cats - k)
        block = lax.rem(cat + k, cats)
        for n in range(fronts):
            group = paired(lax.div(me, strata), turns[n], fronts)
            far_sent[k - 1, n] = picked(cats - k, block, group)
            far_move(k, n).start()
    def deal(n):
        group = paired(lax.div(me, strata), turns[n], fronts)
        owned = near[n]
        for k in range(1, cats):
            far_move(k, n).wait_recv()
            owned += dot(far_got[k - 1, n], weights[lax.rem(cat + cats - k, cats)])
        owned = owned.reshape(strata, share, rank)
        step = steps_of(owned, 1)
        codes = coded(owned, step)
        first = group * strata
        if turns[n] and fronts & (fronts - 1) == 0:
            deal_sent[pl.ds(first, strata)] = codes
            deal_steps[pl.ds(first, strata)] = step
            for i in range(strata):
                for move in deal_moves(first + i, me, first + i):
                    move.start()
        else:
            for i in range(strata):
                stratum = first + i

                @pl.when(stratum == me)
                def _():
                    dealt[me] = codes[i]
                    dealt_steps[me] = step[i]

                @pl.when(stratum != me)
                def _():
                    deal_sent[stratum] = codes[i]
                    deal_steps[stratum] = step[i]
                    for move in deal_moves(stratum, me, stratum):
                        move.start()

    right = lax.rem(me + 1, size)
    chunk = got.shape[2]
    chunks = n_items // chunk
    per = chunk // share
    order = near_first(chunks)
    tiles = n_items // LANES

    def moves(t, n):
        return [
            pltpu.make_async_remote_copy(
                src_ref=src.at[t, n],
                dst_ref=dst.at[t, n],
                send_sem=send_sem.at[t, n, k],
                recv_sem=recv_sem.at[t, n, k],
                device_id={"blk": right},
                device_id_type=MESH,
            )
            for k, (src, dst) in enumerate([(sent, got), (sent_steps, got_steps)])
        ]

    def unpack(piece):
        t, n = divmod(piece, chunks)
        for j in range(chunk // LANES):
            tile = n * (chunk // LANES) + j
            part = ratings[pl.ds(tile * rounds + t, n_users, stride=tiles * rounds), :]
            values[t, n, :, pl.ds(j * LANES, LANES)] = part.astype(jnp.float32).astype(jnp.bfloat16)

    def round_step(t, n, user_parts, kept, grads):
        place = paired(lax.div(lax.rem(me - t + size, size), per), order[n], chunks)
        if t == 0:
            for i in range(per):
                source = place * per + i

                def arrive():
                    for move in deal_moves(source, source, source):
                        move.wait_recv()

                if order[n] and chunks & (chunks - 1) == 0:
                    arrive()
                else:
                    pl.when(source != me)(arrive)

            here = pl.ds(place * per, per)
            old = decoded(dealt[here], dealt_steps[here]).reshape(chunk, rank)
        else:
            for move in moves(t - 1, n):
                move.wait_recv()
            old = decoded(got[t - 1, n], got_steps[t - 1, n])
        old_parts = split(old)
        guess = product(user_parts, old_parts, ((1,), (1,)))
        rated = values[t, place].astype(jnp.float32)
        error_parts = split(jnp.where(rated > 0.0, rated - guess, 0.0))
        if kept:
            grads.append(product(*kept.pop(), ((1,), (0,))))
        item_grad = product(error_parts, user_parts, ((0,), (0,)))
        new = old + learn_rate * (item_grad - shrink * old)
        if t < rounds - 1:
            step = steps_of(new, 0)
            sent[t, n] = coded(new, step)
            sent_steps[t, n] = step
        else:
            items_out[pl.ds(pl.multiple_of(place * chunk, chunk), chunk), :] = new
        if n < chunks - 1:
            kept.append((error_parts, old_parts))
        else:
            grads.append(product(error_parts, old_parts, ((1,), (0,))))
        if t < rounds - 1:
            for move in moves(t, n):
                move.start()

    loads[3].wait()
    loads[4].wait()
    pieces = list(range(rounds * chunks))

    def unpack_some(count):
        for piece in pieces[:count]:
            unpack(piece)
        del pieces[:count]

    early = unpacked_early(rounds * chunks)
    unpack_some(early)
    each = pl.cdiv(len(pieces), fronts)
    now = users[...]
    user_parts = split(now)
    kept, grads = [], []

    def first_round(n):
        round_step(0, n, user_parts, kept, grads)

    for n in range(fronts):
        deal(n)
        unpack_some(each)
    unpack_some(len(pieces))
    for n in range(chunks):
        first_round(n)
    for t in range(rounds):
        if t > 0:
            user_parts, grads = split(now), []
            for n in range(chunks):
                round_step(t, n, user_parts, kept, grads)
        now = now + learn_rate * (functools.reduce(jnp.add, grads) - shrink * now)
    users_out[...] = now

    for k in range(1, cats):
        order_move(k).wait_send()
        for n in range(fronts):
            far_move(k, n).wait_send()

    def settle(stratum, carry):
        @pl.when(stratum != me)
        def _():
            for move in deal_moves(stratum, me, stratum):
                move.wait_send()

        return carry

    lax.fori_loop(0, size, settle, 0)
    for t in range(rounds - 1):
        for n in range(chunks):
            for move in moves(t, n):
                move.wait_send()


def body(item_content, projection, send_order, user_factors, ratings):
    size, cats = lax.axis_size("blk"), lax.axis_size("cat")
    n_users, rounds, n_items = ratings.shape
    width, rank = item_content.shape[1], user_factors.shape[1]
    share = n_items // size
    chunk, front = max(CHUNK, share), max(FRONT, share)
    chunks, fronts = n_items // chunk, n_items // front
    view = ratings.reshape(n_users, rounds, n_items // LANES, LANES).transpose(0, 2, 1, 3).reshape(-1, LANES)
    dma = pltpu.SemaphoreType.DMA
    return tuple(
        pl.pallas_call(
            functools.partial(kernel, rounds),
            in_specs=[pl.BlockSpec(memory_space=pl.ANY)] * 5,
            out_specs=[pl.BlockSpec(memory_space=pltpu.VMEM)] * 2,
            out_shape=[
                jax.ShapeDtypeStruct((n_users, rank), jnp.float32),
                jax.ShapeDtypeStruct((n_items, rank), jnp.float32),
            ],
            scratch_shapes=[
                pltpu.VMEM((cats, n_items, width), jnp.bfloat16),
                pltpu.VMEM((cats, width, rank), jnp.bfloat16),
                pltpu.VMEM((cats, 1, n_items), jnp.int32),
                pltpu.VMEM((cats, n_items, LANES), jnp.float32),
                pltpu.VMEM((fronts, front, rank), jnp.float32),
                pltpu.VMEM((cats - 1, fronts, front, width), jnp.bfloat16),
                pltpu.VMEM((cats - 1, fronts, front, width), jnp.bfloat16),
                pltpu.VMEM((size, share, rank), jnp.int16),
                pltpu.VMEM((size, 1, rank), jnp.float32),
                pltpu.VMEM((size, share, rank), jnp.int16),
                pltpu.VMEM((size, 1, rank), jnp.float32),
                pltpu.VMEM((n_users, rank), jnp.float32),
                pltpu.VMEM(view.shape, jnp.int32),
                pltpu.VMEM((rounds, chunks, n_users, chunk), jnp.bfloat16),
                pltpu.VMEM((rounds - 1, chunks, chunk, rank), jnp.int16),
                pltpu.VMEM((rounds - 1, chunks, 1, rank), jnp.float32),
                pltpu.VMEM((rounds - 1, chunks, chunk, rank), jnp.int16),
                pltpu.VMEM((rounds - 1, chunks, 1, rank), jnp.float32),
                dma((5,)),
                dma((cats - 1,)),
                dma((cats - 1,)),
                dma((cats - 1, fronts)),
                dma((cats - 1, fronts)),
                dma((size, 2)),
                dma((size, 2)),
                dma((rounds - 1, chunks, 2)),
                dma((rounds - 1, chunks, 2)),
            ],
            cost_estimate=pl.CostEstimate(
                flops=18 * n_users * n_items * rank * rounds, bytes_accessed=12 << 20, transcendentals=0
            ),
            compiler_params=pltpu.CompilerParams(
                vmem_limit_bytes=48 << 20, collective_id=0, has_side_effects=True
            ),
            name="stratified_sgd",
        )(
            *[
                pltpu.with_memory_space_constraint(value, pltpu.HBM)
                for value in (
                    item_content.reshape(cats, n_items, width),
                    projection.reshape(cats, width, rank),
                    send_order,
                    user_factors,
                    view,
                )
            ]
        )
    )


def solution(mesh):
    placed = (
        P("blk", "cat"),
        P(),
        P(("blk", "cat"), None),
        P(("blk", "cat"), None),
        P(("blk", "cat"), None, None),
    )
    return jax.shard_map(
        body,
        mesh=mesh,
        in_specs=placed,
        out_specs=(P(("blk", "cat"), None), P(("blk", "cat"), None)),
        check_vma=False,
    )
```

```python
import functools
import jax
import jax.numpy as jnp
from jax import lax
from jax.experimental import pallas as pl
from jax.experimental.pallas import tpu as pltpu
from jax.sharding import PartitionSpec as P

learn_rate = 0.004
shrink = 0.05
LEVELS = 32000.0
CHUNK = 256
FRONT = 256
LANES = 128
MESH = pl.DeviceIdType.MESH


def split(value):
    high = value.astype(jnp.bfloat16)
    return high, (value - high.astype(jnp.float32)).astype(jnp.bfloat16)


def dot(left, right, dims=((1,), (0,))):
    return lax.dot_general(left, right, (dims, ((), ())), preferred_element_type=jnp.float32)


def product(left, right, dims):
    return dot(left[0], right[0], dims) + (dot(left[0], right[1], dims) + dot(left[1], right[0], dims))


def steps_of(value, axis):
    return jnp.maximum(jnp.max(jnp.abs(value), axis=axis, keepdims=True), 1e-30) * (1.0 / LEVELS)


def coded(value, step):
    return jnp.floor(value * (1.0 / step) + 0.5).astype(jnp.int32).astype(jnp.int16)


def decoded(value, step):
    return value.astype(jnp.int32).astype(jnp.float32) * step


def paired(index, turn, count):
    if count & (count - 1):
        return lax.rem(turn - index + count, count)
    result, bit = index, 1
    while bit < count:
        if turn & bit:
            result = result + bit * (1 - 2 * lax.rem(lax.div(index, bit), 2))
        bit *= 2
    return result


def far_first(count):
    half = count // 2
    return list(range(half, count)) + list(range(half - 1, -1, -1))


def near_first(count):
    return [count // 2] + list(range(count // 2 - 1, -1, -1)) + list(range(count // 2 + 1, count))


def unpacked_early(count):
    return count // 4


def kernel(
    rounds, content_in, weights_in, order_in, users_in, ratings_in, users_out, items_out,
    content, weights, orders, column, near, far_sent, far_got,
    deal_sent, deal_steps, dealt, dealt_steps,
    users, ratings, values, sent, sent_steps, got, got_steps,
    load_sem, order_send, order_recv, far_send, far_recv, deal_send, deal_recv, send_sem, recv_sem,
):
    size, cats = lax.axis_size("blk"), lax.axis_size("cat")
    me, cat = lax.axis_index("blk"), lax.axis_index("cat")
    n_users, rank = users.shape
    n_items, width = content.shape[1:]
    share = n_items // size
    loads = [
        pltpu.make_async_copy(src, dst, load_sem.at[k])
        for k, (src, dst) in enumerate(
            [
                (order_in, orders.at[0]),
                (content_in, content),
                (weights_in, weights),
                (users_in, users),
                (ratings_in, ratings),
            ]
        )
    ]
    for load in loads:
        load.start()
    barrier = pltpu.get_barrier_semaphore()
    for k in range(1, cats):
        pl.semaphore_signal(barrier, inc=1, device_id={"cat": lax.rem(cat + k, cats)}, device_id_type=MESH)

    def greet(k, carry):
        pl.semaphore_signal(barrier, inc=1, device_id={"blk": lax.rem(me + k, size)}, device_id_type=MESH)
        return carry

    lax.fori_loop(1, size, greet, 0)

    front = far_sent.shape[2]
    fronts = n_items // front
    strata = front // share
    turns = far_first(fronts)

    def spread(slot):
        row = orders[slot].astype(jnp.float32)
        column[slot] = jnp.transpose(jnp.broadcast_to(row, (LANES, n_items)))

    def picked(slot, block, group):
        at = column[slot, pl.ds(pl.multiple_of(group * front, front), front), :]
        lane = lax.broadcasted_iota(jnp.int32, (front, LANES), 1).astype(jnp.float32)
        hot = jnp.concatenate(
            [jnp.where(at == lane + float(j * LANES), 1.0, 0.0).astype(jnp.bfloat16) for j in range(n_items // LANES)],
            axis=1,
        )
        return dot(hot, content[block]).astype(jnp.bfloat16)

    def near_part(n):
        group = paired(lax.div(me, strata), turns[n], fronts)
        near[n] = dot(picked(0, cat, group), weights[cat])

    loads[0].wait()
    spread(0)
    loads[1].wait()
    loads[2].wait()
    for n in range(fronts // 2):
        near_part(n)
    pl.semaphore_wait(barrier, size - 1 + cats - 1)

    def order_move(k):
        return pltpu.make_async_remote_copy(
            src_ref=order_in,
            dst_ref=orders.at[k],
            send_sem=order_send.at[k - 1],
            recv_sem=order_recv.at[k - 1],
            device_id={"cat": lax.rem(cat + k, cats)},
            device_id_type=MESH,
        )

    def far_move(k, n):
        return pltpu.make_async_remote_copy(
            src_ref=far_sent.at[k - 1, n],
            dst_ref=far_got.at[k - 1, n],
            send_sem=far_send.at[k - 1, n],
            recv_sem=far_recv.at[k - 1, n],
            device_id={"cat": lax.rem(cat + k, cats)},
            device_id_type=MESH,
        )

    def deal_moves(stratum, source, target):
        return [
            pltpu.make_async_remote_copy(
                src_ref=src.at[stratum],
                dst_ref=dst.at[source],
                send_sem=deal_send.at[stratum, k],
                recv_sem=deal_recv.at[source, k],
                device_id={"blk": target},
                device_id_type=MESH,
            )
            for k, (src, dst) in enumerate([(deal_sent, dealt), (deal_steps, dealt_steps)])
        ]

    for k in range(1, cats):
        order_move(k).start()
    for n in range(fronts // 2, fronts):
        near_part(n)
    for k in range(1, cats):
        order_move(cats - k).wait_recv()
        spread(cats - k)
        block = lax.rem(cat + k, cats)
        for n in range(fronts):
            group = paired(lax.div(me, strata), turns[n], fronts)
            far_sent[k - 1, n] = picked(cats - k, block, group)
            far_move(k, n).start()
    def deal(n):
        group = paired(lax.div(me, strata), turns[n], fronts)
        owned = near[n]
        for k in range(1, cats):
            far_move(k, n).wait_recv()
            owned += dot(far_got[k - 1, n], weights[lax.rem(cat + cats - k, cats)])
        owned = owned.reshape(strata, share, rank)
        step = steps_of(owned, 1)
        codes = coded(owned, step)
        first = group * strata
        if turns[n] and fronts & (fronts - 1) == 0:
            deal_sent[pl.ds(first, strata)] = codes
            deal_steps[pl.ds(first, strata)] = step
            for i in range(strata):
                for move in deal_moves(first + i, me, first + i):
                    move.start()
        else:
            for i in range(strata):
                stratum = first + i

                @pl.when(stratum == me)
                def _():
                    dealt[me] = codes[i]
                    dealt_steps[me] = step[i]

                @pl.when(stratum != me)
                def _():
                    deal_sent[stratum] = codes[i]
                    deal_steps[stratum] = step[i]
                    for move in deal_moves(stratum, me, stratum):
                        move.start()

    right = lax.rem(me + 1, size)
    chunk = got.shape[2]
    chunks = n_items // chunk
    per = chunk // share
    order = near_first(chunks)
    tiles = n_items // LANES

    def moves(t, n):
        return [
            pltpu.make_async_remote_copy(
                src_ref=src.at[t, n],
                dst_ref=dst.at[t, n],
                send_sem=send_sem.at[t, n, k],
                recv_sem=recv_sem.at[t, n, k],
                device_id={"blk": right},
                device_id_type=MESH,
            )
            for k, (src, dst) in enumerate([(sent, got), (sent_steps, got_steps)])
        ]

    def unpack(piece):
        t, n = divmod(piece, chunks)
        for j in range(chunk // LANES):
            tile = n * (chunk // LANES) + j
            part = ratings[pl.ds(tile * rounds + t, n_users, stride=tiles * rounds), :]
            values[t, n, pl.ds(j * LANES, LANES), :] = jnp.transpose(part.astype(jnp.float32)).astype(jnp.bfloat16)

    def round_step(t, n, user_parts, kept, grads):
        place = paired(lax.div(lax.rem(me - t + size, size), per), order[n], chunks)
        if t == 0:
            for i in range(per):
                source = place * per + i

                def arrive():
                    for move in deal_moves(source, source, source):
                        move.wait_recv()

                if order[n] and chunks & (chunks - 1) == 0:
                    arrive()
                else:
                    pl.when(source != me)(arrive)

            here = pl.ds(place * per, per)
            old = decoded(dealt[here], dealt_steps[here]).reshape(chunk, rank)
        else:
            for move in moves(t - 1, n):
                move.wait_recv()
            old = decoded(got[t - 1, n], got_steps[t - 1, n])
        old_parts = split(old)
        guess = product(old_parts, user_parts, ((1,), (1,)))
        rated = values[t, place].astype(jnp.float32)
        error_parts = split(jnp.where(rated > 0.0, rated - guess, 0.0))
        if kept:
            grads.append(product(*kept.pop(), ((0,), (0,))))
        item_grad = product(error_parts, user_parts, ((1,), (0,)))
        new = old + learn_rate * (item_grad - shrink * old)
        if t < rounds - 1:
            step = steps_of(new, 0)
            sent[t, n] = coded(new, step)
            sent_steps[t, n] = step
        else:
            items_out[pl.ds(pl.multiple_of(place * chunk, chunk), chunk), :] = new
        if t < rounds - 1:
            for move in moves(t, n):
                move.start()
        if n < chunks - 1:
            kept.append((error_parts, old_parts))
        else:
            grads.append(product(error_parts, old_parts, ((0,), (0,))))

    loads[3].wait()
    loads[4].wait()
    pieces = list(range(rounds * chunks))

    def unpack_some(count):
        for piece in pieces[:count]:
            unpack(piece)
        del pieces[:count]

    early = unpacked_early(rounds * chunks)
    unpack_some(early)
    each = pl.cdiv(len(pieces), fronts)
    now = users[...]
    user_parts = split(now)
    kept, grads = [], []

    def first_round(n):
        round_step(0, n, user_parts, kept, grads)

    for n in range(fronts):
        deal(n)
        unpack_some(each)
    unpack_some(len(pieces))
    for n in range(chunks):
        first_round(n)
    for t in range(rounds):
        if t > 0:
            user_parts, grads = split(now), []
            for n in range(chunks):
                round_step(t, n, user_parts, kept, grads)
        now = now + learn_rate * (functools.reduce(jnp.add, grads) - shrink * now)
    users_out[...] = now

    for k in range(1, cats):
        order_move(k).wait_send()
        for n in range(fronts):
            far_move(k, n).wait_send()

    def settle(stratum, carry):
        @pl.when(stratum != me)
        def _():
            for move in deal_moves(stratum, me, stratum):
                move.wait_send()

        return carry

    lax.fori_loop(0, size, settle, 0)
    for t in range(rounds - 1):
        for n in range(chunks):
            for move in moves(t, n):
                move.wait_send()


def finish(users_in, items_in, users_out, items_out, sem):
    moves = [
        pltpu.make_async_copy(users_in, users_out, sem.at[0]),
        pltpu.make_async_copy(items_in, items_out, sem.at[1]),
    ]
    for move in moves:
        move.start()
    for move in moves:
        move.wait()


def finished(users, items):
    return tuple(
        pl.pallas_call(
            finish,
            in_specs=[pl.BlockSpec(memory_space=pltpu.VMEM)] * 2,
            out_specs=[pl.BlockSpec(memory_space=pltpu.HBM)] * 2,
            out_shape=[jax.ShapeDtypeStruct(value.shape, value.dtype) for value in (users, items)],
            scratch_shapes=[pltpu.SemaphoreType.DMA((2,))],
            compiler_params=pltpu.CompilerParams(vmem_limit_bytes=8 << 20),
            name="finish",
        )(users, items)
    )


def body(item_content, projection, send_order, user_factors, ratings):
    size, cats = lax.axis_size("blk"), lax.axis_size("cat")
    n_users, rounds, n_items = ratings.shape
    width, rank = item_content.shape[1], user_factors.shape[1]
    share = n_items // size
    chunk, front = max(CHUNK, share), max(FRONT, share)
    chunks, fronts = n_items // chunk, n_items // front
    view = ratings.reshape(n_users, rounds, n_items // LANES, LANES).transpose(0, 2, 1, 3).reshape(-1, LANES)
    dma = pltpu.SemaphoreType.DMA
    return finished(
        *pl.pallas_call(
            functools.partial(kernel, rounds),
            in_specs=[pl.BlockSpec(memory_space=pl.ANY)] * 5,
            out_specs=[pl.BlockSpec(memory_space=pltpu.VMEM)] * 2,
            out_shape=[
                jax.ShapeDtypeStruct((n_users, rank), jnp.float32),
                jax.ShapeDtypeStruct((n_items, rank), jnp.float32),
            ],
            scratch_shapes=[
                pltpu.VMEM((cats, n_items, width), jnp.bfloat16),
                pltpu.VMEM((cats, width, rank), jnp.bfloat16),
                pltpu.VMEM((cats, 1, n_items), jnp.int32),
                pltpu.VMEM((cats, n_items, LANES), jnp.float32),
                pltpu.VMEM((fronts, front, rank), jnp.float32),
                pltpu.VMEM((cats - 1, fronts, front, width), jnp.bfloat16),
                pltpu.VMEM((cats - 1, fronts, front, width), jnp.bfloat16),
                pltpu.VMEM((size, share, rank), jnp.int16),
                pltpu.VMEM((size, 1, rank), jnp.float32),
                pltpu.VMEM((size, share, rank), jnp.int16),
                pltpu.VMEM((size, 1, rank), jnp.float32),
                pltpu.VMEM((n_users, rank), jnp.float32),
                pltpu.VMEM(view.shape, jnp.int32),
                pltpu.VMEM((rounds, chunks, chunk, n_users), jnp.bfloat16),
                pltpu.VMEM((rounds - 1, chunks, chunk, rank), jnp.int16),
                pltpu.VMEM((rounds - 1, chunks, 1, rank), jnp.float32),
                pltpu.VMEM((rounds - 1, chunks, chunk, rank), jnp.int16),
                pltpu.VMEM((rounds - 1, chunks, 1, rank), jnp.float32),
                dma((5,)),
                dma((cats - 1,)),
                dma((cats - 1,)),
                dma((cats - 1, fronts)),
                dma((cats - 1, fronts)),
                dma((size, 2)),
                dma((size, 2)),
                dma((rounds - 1, chunks, 2)),
                dma((rounds - 1, chunks, 2)),
            ],
            cost_estimate=pl.CostEstimate(
                flops=18 * n_users * n_items * rank * rounds, bytes_accessed=12 << 20, transcendentals=0
            ),
            compiler_params=pltpu.CompilerParams(
                vmem_limit_bytes=48 << 20, collective_id=0, has_side_effects=True
            ),
            name="stratified_sgd",
        )(
            *[
                pltpu.with_memory_space_constraint(value, pltpu.HBM)
                for value in (
                    item_content.reshape(cats, n_items, width),
                    projection.reshape(cats, width, rank),
                    send_order,
                    user_factors,
                    view,
                )
            ]
        )
    )


def solution(mesh):
    placed = (
        P("blk", "cat"),
        P(),
        P(("blk", "cat"), None),
        P(("blk", "cat"), None),
        P(("blk", "cat"), None, None),
    )
    return jax.shard_map(
        body,
        mesh=mesh,
        in_specs=placed,
        out_specs=(P(("blk", "cat"), None), P(("blk", "cat"), None)),
        check_vma=False,
    )
```

```python
import functools
import jax
import jax.numpy as jnp
from jax import lax
from jax.experimental import pallas as pl
from jax.experimental.pallas import tpu as pltpu
from jax.sharding import PartitionSpec as P

learn_rate = 0.004
shrink = 0.05
LEVELS = 32000.0
CHUNK = 256
FRONT = 256
LANES = 128
MESH = pl.DeviceIdType.MESH


def split(value):
    high = value.astype(jnp.bfloat16)
    return high, (value - high.astype(jnp.float32)).astype(jnp.bfloat16)


def dot(left, right, dims=((1,), (0,))):
    return lax.dot_general(left, right, (dims, ((), ())), preferred_element_type=jnp.float32)


def product(left, right, dims):
    return dot(left[0], right[0], dims) + (dot(left[0], right[1], dims) + dot(left[1], right[0], dims))


def steps_of(value, axis):
    return jnp.maximum(jnp.max(jnp.abs(value), axis=axis, keepdims=True), 1e-30) * (1.0 / LEVELS)


def coded(value, step):
    return jnp.floor(value * (1.0 / step) + 0.5).astype(jnp.int32).astype(jnp.int16)


def decoded(value, step):
    return value.astype(jnp.int32).astype(jnp.float32) * step


def paired(index, turn, count):
    if count & (count - 1):
        return lax.rem(turn - index + count, count)
    result, bit = index, 1
    while bit < count:
        if turn & bit:
            result = result + bit * (1 - 2 * lax.rem(lax.div(index, bit), 2))
        bit *= 2
    return result


def alternate(count):
    half, turns = count // 2, []
    for i in range(count - half):
        turns.append(half + i)
        if i < half:
            turns.append(half - 1 - i)
    return turns


def unpacked_early(count):
    return count // 4


def kernel(
    rounds, content_in, weights_in, order_in, users_in, ratings_in, users_out, items_out,
    content, weights, orders, column, near, far_sent, far_got,
    deal_sent, deal_steps, dealt, dealt_steps,
    users, ratings, values, sent, sent_steps, got, got_steps,
    load_sem, order_send, order_recv, far_send, far_recv, deal_send, deal_recv, send_sem, recv_sem,
):
    size, cats = lax.axis_size("blk"), lax.axis_size("cat")
    me, cat = lax.axis_index("blk"), lax.axis_index("cat")
    n_users, rank = users.shape
    n_items, width = content.shape[1:]
    share = n_items // size
    loads = [
        pltpu.make_async_copy(src, dst, load_sem.at[k])
        for k, (src, dst) in enumerate(
            [
                (order_in, orders.at[0]),
                (content_in, content),
                (weights_in, weights),
                (users_in, users),
                (ratings_in, ratings),
            ]
        )
    ]
    for load in loads:
        load.start()
    barrier = pltpu.get_barrier_semaphore()
    for k in range(1, cats):
        pl.semaphore_signal(barrier, inc=1, device_id={"cat": lax.rem(cat + k, cats)}, device_id_type=MESH)

    def greet(k, carry):
        pl.semaphore_signal(barrier, inc=1, device_id={"blk": lax.rem(me + k, size)}, device_id_type=MESH)
        return carry

    lax.fori_loop(1, size, greet, 0)

    front = far_sent.shape[2]
    fronts = n_items // front
    strata = front // share
    turns = alternate(fronts)

    def spread(slot):
        row = orders[slot].astype(jnp.float32)
        column[slot] = jnp.transpose(jnp.broadcast_to(row, (LANES, n_items)))

    def picked(slot, block, group):
        at = column[slot, pl.ds(pl.multiple_of(group * front, front), front), :]
        lane = lax.broadcasted_iota(jnp.int32, (front, LANES), 1).astype(jnp.float32)
        hot = jnp.concatenate(
            [jnp.where(at == lane + float(j * LANES), 1.0, 0.0).astype(jnp.bfloat16) for j in range(n_items // LANES)],
            axis=1,
        )
        return dot(hot, content[block]).astype(jnp.bfloat16)

    def near_part(n):
        group = paired(lax.div(me, strata), turns[n], fronts)
        near[n] = dot(picked(0, cat, group), weights[cat])

    loads[0].wait()
    spread(0)
    loads[1].wait()
    loads[2].wait()
    for n in range(fronts // 2):
        near_part(n)
    pl.semaphore_wait(barrier, size - 1 + cats - 1)

    def order_move(k):
        return pltpu.make_async_remote_copy(
            src_ref=order_in,
            dst_ref=orders.at[k],
            send_sem=order_send.at[k - 1],
            recv_sem=order_recv.at[k - 1],
            device_id={"cat": lax.rem(cat + k, cats)},
            device_id_type=MESH,
        )

    def far_move(k, n):
        return pltpu.make_async_remote_copy(
            src_ref=far_sent.at[k - 1, n],
            dst_ref=far_got.at[k - 1, n],
            send_sem=far_send.at[k - 1, n],
            recv_sem=far_recv.at[k - 1, n],
            device_id={"cat": lax.rem(cat + k, cats)},
            device_id_type=MESH,
        )

    def deal_moves(stratum, source, target):
        return [
            pltpu.make_async_remote_copy(
                src_ref=src.at[stratum],
                dst_ref=dst.at[source],
                send_sem=deal_send.at[stratum, k],
                recv_sem=deal_recv.at[source, k],
                device_id={"blk": target},
                device_id_type=MESH,
            )
            for k, (src, dst) in enumerate([(deal_sent, dealt), (deal_steps, dealt_steps)])
        ]

    for k in range(1, cats):
        order_move(k).start()
    for n in range(fronts // 2, fronts):
        near_part(n)
    for k in range(1, cats):
        order_move(cats - k).wait_recv()
        spread(cats - k)
        block = lax.rem(cat + k, cats)
        for n in range(fronts):
            group = paired(lax.div(me, strata), turns[n], fronts)
            far_sent[k - 1, n] = picked(cats - k, block, group)
            far_move(k, n).start()
    def deal(n):
        group = paired(lax.div(me, strata), turns[n], fronts)
        owned = near[n]
        for k in range(1, cats):
            far_move(k, n).wait_recv()
            owned += dot(far_got[k - 1, n], weights[lax.rem(cat + cats - k, cats)])
        owned = owned.reshape(strata, share, rank)
        step = steps_of(owned, 1)
        codes = coded(owned, step)
        first = group * strata
        if turns[n] and fronts & (fronts - 1) == 0:
            deal_sent[pl.ds(first, strata)] = codes
            deal_steps[pl.ds(first, strata)] = step
            for i in range(strata):
                for move in deal_moves(first + i, me, first + i):
                    move.start()
        else:
            for i in range(strata):
                stratum = first + i

                @pl.when(stratum == me)
                def _():
                    dealt[me] = codes[i]
                    dealt_steps[me] = step[i]

                @pl.when(stratum != me)
                def _():
                    deal_sent[stratum] = codes[i]
                    deal_steps[stratum] = step[i]
                    for move in deal_moves(stratum, me, stratum):
                        move.start()

    right = lax.rem(me + 1, size)
    chunk = got.shape[2]
    chunks = n_items // chunk
    per = chunk // share
    order = alternate(chunks)
    tiles = n_items // LANES

    def moves(t, n):
        return [
            pltpu.make_async_remote_copy(
                src_ref=src.at[t, n],
                dst_ref=dst.at[t, n],
                send_sem=send_sem.at[t, n, k],
                recv_sem=recv_sem.at[t, n, k],
                device_id={"blk": right},
                device_id_type=MESH,
            )
            for k, (src, dst) in enumerate([(sent, got), (sent_steps, got_steps)])
        ]

    def unpack(piece):
        t, n = divmod(piece, chunks)
        for j in range(chunk // LANES):
            tile = n * (chunk // LANES) + j
            part = ratings[pl.ds(tile * rounds + t, n_users, stride=tiles * rounds), :]
            values[t, n, pl.ds(j * LANES, LANES), :] = jnp.transpose(part.astype(jnp.float32)).astype(jnp.bfloat16)

    def round_step(t, n, user_parts, kept, grads):
        place = paired(lax.div(lax.rem(me - t + size, size), per), order[n], chunks)
        if t == 0:
            for i in range(per):
                source = place * per + i

                def arrive():
                    for move in deal_moves(source, source, source):
                        move.wait_recv()

                if order[n] and chunks & (chunks - 1) == 0:
                    arrive()
                else:
                    pl.when(source != me)(arrive)

            here = pl.ds(place * per, per)
            old = decoded(dealt[here], dealt_steps[here]).reshape(chunk, rank)
        else:
            for move in moves(t - 1, n):
                move.wait_recv()
            old = decoded(got[t - 1, n], got_steps[t - 1, n])
        old_parts = split(old)
        guess = product(old_parts, user_parts, ((1,), (1,)))
        rated = values[t, place].astype(jnp.float32)
        error_parts = split(jnp.where(rated > 0.0, rated - guess, 0.0))
        if kept:
            grads.append(product(*kept.pop(), ((0,), (0,))))
        item_grad = product(error_parts, user_parts, ((1,), (0,)))
        new = old + learn_rate * (item_grad - shrink * old)
        if t < rounds - 1:
            step = steps_of(new, 0)
            sent[t, n] = coded(new, step)
            sent_steps[t, n] = step
        else:
            items_out[pl.ds(pl.multiple_of(place * chunk, chunk), chunk), :] = new
        if t < rounds - 1:
            for move in moves(t, n):
                move.start()
        if n < chunks - 1:
            kept.append((error_parts, old_parts))
        else:
            grads.append(product(error_parts, old_parts, ((0,), (0,))))

    loads[3].wait()
    loads[4].wait()
    pieces = list(range(rounds * chunks))

    def unpack_some(count):
        for piece in pieces[:count]:
            unpack(piece)
        del pieces[:count]

    early = unpacked_early(rounds * chunks)
    unpack_some(early)
    each = pl.cdiv(len(pieces), fronts)
    now = users[...]
    user_parts = split(now)
    kept, grads = [], []

    def first_round(n):
        round_step(0, n, user_parts, kept, grads)

    for n in range(fronts):
        deal(n)
        unpack_some(each)
    unpack_some(len(pieces))
    for n in range(chunks):
        first_round(n)
    for t in range(rounds):
        if t > 0:
            user_parts, grads = split(now), []
            for n in range(chunks):
                round_step(t, n, user_parts, kept, grads)
        now = now + learn_rate * (functools.reduce(jnp.add, grads) - shrink * now)
    users_out[...] = now

    for k in range(1, cats):
        order_move(k).wait_send()
        for n in range(fronts):
            far_move(k, n).wait_send()

    def settle(stratum, carry):
        @pl.when(stratum != me)
        def _():
            for move in deal_moves(stratum, me, stratum):
                move.wait_send()

        return carry

    lax.fori_loop(0, size, settle, 0)
    for t in range(rounds - 1):
        for n in range(chunks):
            for move in moves(t, n):
                move.wait_send()


def finish(users_in, items_in, users_out, items_out, sem):
    moves = [
        pltpu.make_async_copy(users_in, users_out, sem.at[0]),
        pltpu.make_async_copy(items_in, items_out, sem.at[1]),
    ]
    for move in moves:
        move.start()
    for move in moves:
        move.wait()


def finished(users, items):
    return tuple(
        pl.pallas_call(
            finish,
            in_specs=[pl.BlockSpec(memory_space=pltpu.VMEM)] * 2,
            out_specs=[pl.BlockSpec(memory_space=pltpu.HBM)] * 2,
            out_shape=[jax.ShapeDtypeStruct(value.shape, value.dtype) for value in (users, items)],
            scratch_shapes=[pltpu.SemaphoreType.DMA((2,))],
            compiler_params=pltpu.CompilerParams(vmem_limit_bytes=8 << 20),
            name="finish",
        )(users, items)
    )


def body(item_content, projection, send_order, user_factors, ratings):
    size, cats = lax.axis_size("blk"), lax.axis_size("cat")
    n_users, rounds, n_items = ratings.shape
    width, rank = item_content.shape[1], user_factors.shape[1]
    share = n_items // size
    chunk, front = max(CHUNK, share), max(FRONT, share)
    chunks, fronts = n_items // chunk, n_items // front
    view = ratings.reshape(n_users, rounds, n_items // LANES, LANES).transpose(0, 2, 1, 3).reshape(-1, LANES)
    dma = pltpu.SemaphoreType.DMA
    return finished(
        *pl.pallas_call(
            functools.partial(kernel, rounds),
            in_specs=[pl.BlockSpec(memory_space=pl.ANY)] * 5,
            out_specs=[pl.BlockSpec(memory_space=pltpu.VMEM)] * 2,
            out_shape=[
                jax.ShapeDtypeStruct((n_users, rank), jnp.float32),
                jax.ShapeDtypeStruct((n_items, rank), jnp.float32),
            ],
            scratch_shapes=[
                pltpu.VMEM((cats, n_items, width), jnp.bfloat16),
                pltpu.VMEM((cats, width, rank), jnp.bfloat16),
                pltpu.VMEM((cats, 1, n_items), jnp.int32),
                pltpu.VMEM((cats, n_items, LANES), jnp.float32),
                pltpu.VMEM((fronts, front, rank), jnp.float32),
                pltpu.VMEM((cats - 1, fronts, front, width), jnp.bfloat16),
                pltpu.VMEM((cats - 1, fronts, front, width), jnp.bfloat16),
                pltpu.VMEM((size, share, rank), jnp.int16),
                pltpu.VMEM((size, 1, rank), jnp.float32),
                pltpu.VMEM((size, share, rank), jnp.int16),
                pltpu.VMEM((size, 1, rank), jnp.float32),
                pltpu.VMEM((n_users, rank), jnp.float32),
                pltpu.VMEM(view.shape, jnp.int32),
                pltpu.VMEM((rounds, chunks, chunk, n_users), jnp.bfloat16),
                pltpu.VMEM((rounds - 1, chunks, chunk, rank), jnp.int16),
                pltpu.VMEM((rounds - 1, chunks, 1, rank), jnp.float32),
                pltpu.VMEM((rounds - 1, chunks, chunk, rank), jnp.int16),
                pltpu.VMEM((rounds - 1, chunks, 1, rank), jnp.float32),
                dma((5,)),
                dma((cats - 1,)),
                dma((cats - 1,)),
                dma((cats - 1, fronts)),
                dma((cats - 1, fronts)),
                dma((size, 2)),
                dma((size, 2)),
                dma((rounds - 1, chunks, 2)),
                dma((rounds - 1, chunks, 2)),
            ],
            cost_estimate=pl.CostEstimate(
                flops=18 * n_users * n_items * rank * rounds, bytes_accessed=12 << 20, transcendentals=0
            ),
            compiler_params=pltpu.CompilerParams(
                vmem_limit_bytes=48 << 20, collective_id=0, has_side_effects=True
            ),
            name="stratified_sgd",
        )(
            *[
                pltpu.with_memory_space_constraint(value, pltpu.HBM)
                for value in (
                    item_content.reshape(cats, n_items, width),
                    projection.reshape(cats, width, rank),
                    send_order,
                    user_factors,
                    view,
                )
            ]
        )
    )


def solution(mesh):
    placed = (
        P("blk", "cat"),
        P(),
        P(("blk", "cat"), None),
        P(("blk", "cat"), None),
        P(("blk", "cat"), None, None),
    )
    return jax.shard_map(
        body,
        mesh=mesh,
        in_specs=placed,
        out_specs=(P(("blk", "cat"), None), P(("blk", "cat"), None)),
        check_vma=False,
    )
```

```python
import functools
import jax
import jax.numpy as jnp
from jax import lax
from jax.experimental import pallas as pl
from jax.experimental.pallas import tpu as pltpu
from jax.sharding import PartitionSpec as P

learn_rate = 0.004
shrink = 0.05
LEVELS = 32000.0
CHUNK = 256
FRONT = 256
LANES = 128
MESH = pl.DeviceIdType.MESH


def split(value):
    high = value.astype(jnp.bfloat16)
    return high, (value - high.astype(jnp.float32)).astype(jnp.bfloat16)


def dot(left, right, dims=((1,), (0,))):
    return lax.dot_general(left, right, (dims, ((), ())), preferred_element_type=jnp.float32)


def product(left, right, dims):
    return dot(left[0], right[0], dims) + (dot(left[0], right[1], dims) + dot(left[1], right[0], dims))


def steps_of(value, axis):
    return jnp.maximum(jnp.max(jnp.abs(value), axis=axis, keepdims=True), 1e-30) * (1.0 / LEVELS)


def coded(value, step):
    return jnp.floor(value * (1.0 / step) + 0.5).astype(jnp.int32).astype(jnp.int16)


def decoded(value, step):
    return value.astype(jnp.int32).astype(jnp.float32) * step


def paired(index, turn, count):
    if count & (count - 1):
        return lax.rem(turn - index + count, count)
    result, bit = index, 1
    while bit < count:
        if turn & bit:
            result = result + bit * (1 - 2 * lax.rem(lax.div(index, bit), 2))
        bit *= 2
    return result


def alternate(count):
    half, turns = count // 2, []
    for i in range(count - half):
        turns.append(half + i)
        if i < half:
            turns.append(half - 1 - i)
    return turns


def unpacked_early(count):
    return count * 5 // 8


def kernel(
    rounds, content_in, weights_in, order_in, users_in, ratings_in, users_out, items_out,
    content, weights, orders, column, near, far_sent, far_got,
    deal_sent, deal_steps, dealt, dealt_steps,
    users, ratings, values, sent, sent_steps, got, got_steps,
    load_sem, order_send, order_recv, far_send, far_recv, deal_send, deal_recv, send_sem, recv_sem,
):
    size, cats = lax.axis_size("blk"), lax.axis_size("cat")
    me, cat = lax.axis_index("blk"), lax.axis_index("cat")
    n_users, rank = users.shape
    n_items, width = content.shape[1:]
    share = n_items // size
    loads = [
        pltpu.make_async_copy(src, dst, load_sem.at[k])
        for k, (src, dst) in enumerate(
            [
                (order_in, orders.at[0]),
                (content_in, content),
                (weights_in, weights),
                (users_in, users),
                (ratings_in, ratings),
            ]
        )
    ]
    for load in loads:
        load.start()
    barrier = pltpu.get_barrier_semaphore()
    for k in range(1, cats):
        pl.semaphore_signal(barrier, inc=1, device_id={"cat": lax.rem(cat + k, cats)}, device_id_type=MESH)

    def greet(k, carry):
        pl.semaphore_signal(barrier, inc=1, device_id={"blk": lax.rem(me + k, size)}, device_id_type=MESH)
        return carry

    lax.fori_loop(1, size, greet, 0)

    front = far_sent.shape[2]
    fronts = n_items // front
    strata = front // share
    turns = alternate(fronts)

    def spread(slot):
        row = orders[slot].astype(jnp.float32)
        column[slot] = jnp.transpose(jnp.broadcast_to(row, (LANES, n_items)))

    def picked(slot, block, group):
        at = column[slot, pl.ds(pl.multiple_of(group * front, front), front), :]
        lane = lax.broadcasted_iota(jnp.int32, (front, LANES), 1).astype(jnp.float32)
        hot = jnp.concatenate(
            [jnp.where(at == lane + float(j * LANES), 1.0, 0.0).astype(jnp.bfloat16) for j in range(n_items // LANES)],
            axis=1,
        )
        return dot(hot, content[block]).astype(jnp.bfloat16)

    def near_part(n):
        group = paired(lax.div(me, strata), turns[n], fronts)
        near[n] = dot(picked(0, cat, group), weights[cat])

    loads[0].wait()
    spread(0)
    loads[1].wait()
    loads[2].wait()
    for n in range(fronts // 2):
        near_part(n)
    pl.semaphore_wait(barrier, size - 1 + cats - 1)

    def order_move(k):
        return pltpu.make_async_remote_copy(
            src_ref=order_in,
            dst_ref=orders.at[k],
            send_sem=order_send.at[k - 1],
            recv_sem=order_recv.at[k - 1],
            device_id={"cat": lax.rem(cat + k, cats)},
            device_id_type=MESH,
        )

    def far_move(k, n):
        return pltpu.make_async_remote_copy(
            src_ref=far_sent.at[k - 1, n],
            dst_ref=far_got.at[k - 1, n],
            send_sem=far_send.at[k - 1, n],
            recv_sem=far_recv.at[k - 1, n],
            device_id={"cat": lax.rem(cat + k, cats)},
            device_id_type=MESH,
        )

    def deal_moves(stratum, source, target):
        return [
            pltpu.make_async_remote_copy(
                src_ref=src.at[stratum],
                dst_ref=dst.at[source],
                send_sem=deal_send.at[stratum, k],
                recv_sem=deal_recv.at[source, k],
                device_id={"blk": target},
                device_id_type=MESH,
            )
            for k, (src, dst) in enumerate([(deal_sent, dealt), (deal_steps, dealt_steps)])
        ]

    for k in range(1, cats):
        order_move(k).start()
    for n in range(fronts // 2, fronts):
        near_part(n)
    for k in range(1, cats):
        order_move(cats - k).wait_recv()
        spread(cats - k)
        block = lax.rem(cat + k, cats)
        for n in range(fronts):
            group = paired(lax.div(me, strata), turns[n], fronts)
            far_sent[k - 1, n] = picked(cats - k, block, group)
            far_move(k, n).start()
    def deal(n):
        group = paired(lax.div(me, strata), turns[n], fronts)
        owned = near[n]
        for k in range(1, cats):
            far_move(k, n).wait_recv()
            owned += dot(far_got[k - 1, n], weights[lax.rem(cat + cats - k, cats)])
        owned = owned.reshape(strata, share, rank)
        step = steps_of(owned, 1)
        codes = coded(owned, step)
        first = group * strata
        if turns[n] and fronts & (fronts - 1) == 0:
            deal_sent[pl.ds(first, strata)] = codes
            deal_steps[pl.ds(first, strata)] = step
            for i in range(strata):
                for move in deal_moves(first + i, me, first + i):
                    move.start()
        else:
            for i in range(strata):
                stratum = first + i

                @pl.when(stratum == me)
                def _():
                    dealt[me] = codes[i]
                    dealt_steps[me] = step[i]

                @pl.when(stratum != me)
                def _():
                    deal_sent[stratum] = codes[i]
                    deal_steps[stratum] = step[i]
                    for move in deal_moves(stratum, me, stratum):
                        move.start()

    right = lax.rem(me + 1, size)
    chunk = got.shape[2]
    chunks = n_items // chunk
    per = chunk // share
    order = alternate(chunks)
    tiles = n_items // LANES

    def moves(t, n):
        return [
            pltpu.make_async_remote_copy(
                src_ref=src.at[t, n],
                dst_ref=dst.at[t, n],
                send_sem=send_sem.at[t, n, k],
                recv_sem=recv_sem.at[t, n, k],
                device_id={"blk": right},
                device_id_type=MESH,
            )
            for k, (src, dst) in enumerate([(sent, got), (sent_steps, got_steps)])
        ]

    def unpack(piece):
        t, n = divmod(piece, chunks)
        for j in range(chunk // LANES):
            tile = n * (chunk // LANES) + j
            part = ratings[pl.ds(tile * rounds + t, n_users, stride=tiles * rounds), :]
            values[t, n, pl.ds(j * LANES, LANES), :] = jnp.transpose(part.astype(jnp.float32)).astype(jnp.bfloat16)

    def round_step(t, n, user_parts, kept, grads):
        place = paired(lax.div(lax.rem(me - t + size, size), per), order[n], chunks)
        if t == 0:
            for i in range(per):
                source = place * per + i

                def arrive():
                    for move in deal_moves(source, source, source):
                        move.wait_recv()

                if order[n] and chunks & (chunks - 1) == 0:
                    arrive()
                else:
                    pl.when(source != me)(arrive)

            here = pl.ds(place * per, per)
            old = decoded(dealt[here], dealt_steps[here]).reshape(chunk, rank)
        else:
            for move in moves(t - 1, n):
                move.wait_recv()
            old = decoded(got[t - 1, n], got_steps[t - 1, n])
        old_parts = split(old)
        guess = product(old_parts, user_parts, ((1,), (1,)))
        rated = values[t, place].astype(jnp.float32)
        error_parts = split(jnp.where(rated > 0.0, rated - guess, 0.0))
        if kept:
            grads.append(product(*kept.pop(), ((0,), (0,))))
        item_grad = product(error_parts, user_parts, ((1,), (0,)))
        new = old + learn_rate * (item_grad - shrink * old)
        if t < rounds - 1:
            step = steps_of(new, 0)
            sent[t, n] = coded(new, step)
            sent_steps[t, n] = step
        else:
            items_out[pl.ds(pl.multiple_of(place * chunk, chunk), chunk), :] = new
        if t < rounds - 1:
            for move in moves(t, n):
                move.start()
        if n < chunks - 1:
            kept.append((error_parts, old_parts))
        else:
            grads.append(product(error_parts, old_parts, ((0,), (0,))))

    loads[3].wait()
    loads[4].wait()
    pieces = list(range(rounds * chunks))

    def unpack_some(count):
        for piece in pieces[:count]:
            unpack(piece)
        del pieces[:count]

    early = unpacked_early(rounds * chunks)
    unpack_some(early)
    each = pl.cdiv(len(pieces), fronts)
    now = users[...]
    user_parts = split(now)
    kept, grads = [], []

    def first_round(n):
        round_step(0, n, user_parts, kept, grads)

    for n in range(fronts):
        deal(n)
        unpack_some(each)
    unpack_some(len(pieces))
    for n in range(chunks):
        first_round(n)
    for t in range(rounds):
        if t > 0:
            user_parts, grads = split(now), []
            for n in range(chunks):
                round_step(t, n, user_parts, kept, grads)
        now = now + learn_rate * (functools.reduce(jnp.add, grads) - shrink * now)
    users_out[...] = now

    for k in range(1, cats):
        order_move(k).wait_send()
        for n in range(fronts):
            far_move(k, n).wait_send()

    def settle(stratum, carry):
        @pl.when(stratum != me)
        def _():
            for move in deal_moves(stratum, me, stratum):
                move.wait_send()

        return carry

    lax.fori_loop(0, size, settle, 0)
    for t in range(rounds - 1):
        for n in range(chunks):
            for move in moves(t, n):
                move.wait_send()


def finish(users_in, items_in, users_out, items_out, sem):
    moves = [
        pltpu.make_async_copy(users_in, users_out, sem.at[0]),
        pltpu.make_async_copy(items_in, items_out, sem.at[1]),
    ]
    for move in moves:
        move.start()
    for move in moves:
        move.wait()


def finished(users, items):
    return tuple(
        pl.pallas_call(
            finish,
            in_specs=[pl.BlockSpec(memory_space=pltpu.VMEM)] * 2,
            out_specs=[pl.BlockSpec(memory_space=pltpu.HBM)] * 2,
            out_shape=[jax.ShapeDtypeStruct(value.shape, value.dtype) for value in (users, items)],
            scratch_shapes=[pltpu.SemaphoreType.DMA((2,))],
            compiler_params=pltpu.CompilerParams(vmem_limit_bytes=8 << 20),
            name="finish",
        )(users, items)
    )


def body(item_content, projection, send_order, user_factors, ratings):
    size, cats = lax.axis_size("blk"), lax.axis_size("cat")
    n_users, rounds, n_items = ratings.shape
    width, rank = item_content.shape[1], user_factors.shape[1]
    share = n_items // size
    chunk, front = max(CHUNK, share), max(FRONT, share)
    chunks, fronts = n_items // chunk, n_items // front
    view = ratings.reshape(n_users, rounds, n_items // LANES, LANES).transpose(0, 2, 1, 3).reshape(-1, LANES)
    dma = pltpu.SemaphoreType.DMA
    return finished(
        *pl.pallas_call(
            functools.partial(kernel, rounds),
            in_specs=[pl.BlockSpec(memory_space=pl.ANY)] * 5,
            out_specs=[pl.BlockSpec(memory_space=pltpu.VMEM)] * 2,
            out_shape=[
                jax.ShapeDtypeStruct((n_users, rank), jnp.float32),
                jax.ShapeDtypeStruct((n_items, rank), jnp.float32),
            ],
            scratch_shapes=[
                pltpu.VMEM((cats, n_items, width), jnp.bfloat16),
                pltpu.VMEM((cats, width, rank), jnp.bfloat16),
                pltpu.VMEM((cats, 1, n_items), jnp.int32),
                pltpu.VMEM((cats, n_items, LANES), jnp.float32),
                pltpu.VMEM((fronts, front, rank), jnp.float32),
                pltpu.VMEM((cats - 1, fronts, front, width), jnp.bfloat16),
                pltpu.VMEM((cats - 1, fronts, front, width), jnp.bfloat16),
                pltpu.VMEM((size, share, rank), jnp.int16),
                pltpu.VMEM((size, 1, rank), jnp.float32),
                pltpu.VMEM((size, share, rank), jnp.int16),
                pltpu.VMEM((size, 1, rank), jnp.float32),
                pltpu.VMEM((n_users, rank), jnp.float32),
                pltpu.VMEM(view.shape, jnp.int32),
                pltpu.VMEM((rounds, chunks, chunk, n_users), jnp.bfloat16),
                pltpu.VMEM((rounds - 1, chunks, chunk, rank), jnp.int16),
                pltpu.VMEM((rounds - 1, chunks, 1, rank), jnp.float32),
                pltpu.VMEM((rounds - 1, chunks, chunk, rank), jnp.int16),
                pltpu.VMEM((rounds - 1, chunks, 1, rank), jnp.float32),
                dma((5,)),
                dma((cats - 1,)),
                dma((cats - 1,)),
                dma((cats - 1, fronts)),
                dma((cats - 1, fronts)),
                dma((size, 2)),
                dma((size, 2)),
                dma((rounds - 1, chunks, 2)),
                dma((rounds - 1, chunks, 2)),
            ],
            cost_estimate=pl.CostEstimate(
                flops=18 * n_users * n_items * rank * rounds, bytes_accessed=12 << 20, transcendentals=0
            ),
            compiler_params=pltpu.CompilerParams(
                vmem_limit_bytes=48 << 20, collective_id=0, has_side_effects=True
            ),
            name="stratified_sgd",
        )(
            *[
                pltpu.with_memory_space_constraint(value, pltpu.HBM)
                for value in (
                    item_content.reshape(cats, n_items, width),
                    projection.reshape(cats, width, rank),
                    send_order,
                    user_factors,
                    view,
                )
            ]
        )
    )


def solution(mesh):
    placed = (
        P("blk", "cat"),
        P(),
        P(("blk", "cat"), None),
        P(("blk", "cat"), None),
        P(("blk", "cat"), None, None),
    )
    return jax.shard_map(
        body,
        mesh=mesh,
        in_specs=placed,
        out_specs=(P(("blk", "cat"), None), P(("blk", "cat"), None)),
        check_vma=False,
    )
```
